32 devices in a mesh: half: 2 (over core), row: 4 (over y, x), col: 4 (over z).
Axes of the slice: x: 2, y: 2, z: 4, core: 2. Of those that a mesh axis runs over, the one named last changes fastest.
Arguments:
- particles: bfloat16 [64, 2, 64, 4096], P(('half', 'row', 'col')), may hold values from -9 to 9
- orient_bin: int32 [64], P(('half', 'row', 'col')), may hold values from 0 to 15
- tilt_slope: int32 [64, 2], P(('half', 'row', 'col')), may hold values from 12 to 40
- interp_table: bfloat16 [16, 3, 64, 64], replicated, may hold values from 0 to 1.6, as said below
Outputs:
- half_maps: float32 [2, 2, 64, 4096], P('half', None, 'row', 'col')
- shell_power: float32 [2, 29], replicated
- shell_correlation: float32 [2, 29], P('half')
The draws below stay inside these ranges and needn't reach their ends.
Inputs may be any that keep to these rules, and one draw needn't show every extreme that they name: `interp_table`: nonnegative entries.
All inputs are finite; a program needn't handle non-finite values.
Results may differ from the reference program's by a relative error of at most 0.00063.
Values sent between devices are 32-bit elements; how exact they have to be, the bound alone decides.
A program may use at most 64 MiB of HBM per device.

```python
import jax
import jax.numpy as jnp
from jax import lax

GRID = 64
BINS = 16
SHELLS = 29
PARTICLES = 64


def draw_particles(key, part):
    full_shape = (PARTICLES, 2, GRID, GRID * GRID)
    signal = jax.random.normal(jax.random.fold_in(key, 11), (1, 2, GRID, GRID * GRID), jnp.float32)
    noise_part = jax.random.normal(key, full_shape, jnp.float32)
    combined = 0.7 * signal + noise_part
    return jnp.clip(combined, -9.0, 9.0).astype(jnp.bfloat16)


def draw_interp_table(key, part):
    full_shape = (BINS, 3, GRID, GRID)
    row_index = jnp.arange(GRID)[:, None]
    col_index = jnp.arange(GRID)[None, :]
    offset = jnp.abs(row_index - col_index)
    key_diagonal = jax.random.fold_in(key, 21)
    key_band = jax.random.fold_in(key, 22)
    key_dense = jax.random.fold_in(key, 23)
    diagonal_part = jax.random.uniform(key_diagonal, full_shape, jnp.float32, 0.8, 1.2)
    band_part = jax.random.uniform(key_band, full_shape, jnp.float32, 0.03, 0.25)
    dense_part = jax.random.uniform(key_dense, full_shape, jnp.float32, 0.0, 0.02)
    table = jnp.where(offset == 0, diagonal_part, jnp.where(offset <= 2, band_part, 0.0)) + dense_part
    return table.astype(jnp.bfloat16)


def set_ends(result, stream_key, least, high):
    index_at = [jax.random.randint(jax.random.fold_in(stream_key, axis), (), 0, length) for axis, length in enumerate(result.shape)]
    main_axis = result.shape.index(max(result.shape))
    beside = index_at[:main_axis] + [(index_at[main_axis] + 1) % result.shape[main_axis]] + index_at[main_axis + 1:]
    return result.at[tuple(index_at)].set(least).at[tuple(beside)].set(high)


def setup_inputs(seed: int = 0) -> dict:
    keys = jax.random.split(jax.random.key(seed), 5)
    particles = draw_particles(jax.random.fold_in(keys[4], 71), 0)
    orient_bin = set_ends(jax.random.randint(keys[1], (PARTICLES,), 0, BINS), jax.random.fold_in(keys[1], 1), 0, BINS - 1).astype(jnp.int32)
    tilt_slope = set_ends(jax.random.randint(keys[2], (PARTICLES, 2), 12, 41), jax.random.fold_in(keys[2], 1), 12, 40).astype(jnp.int32)
    interp_table = draw_interp_table(jax.random.fold_in(keys[4], 71), 0)
    return dict(particles=particles, orient_bin=orient_bin, tilt_slope=tilt_slope, interp_table=interp_table)


def wedge_mask(tilt_limits, grid_size):
    centre = grid_size // 2
    wave_first = (jnp.arange(grid_size, dtype=jnp.int32) - centre)[:, None]
    wave_third = (jnp.arange(grid_size * grid_size, dtype=jnp.int32) % grid_size - centre)[None, :]
    tilt_limit = jnp.where(wave_first * wave_third >= 0, tilt_limits[0], tilt_limits[1])
    inside = 16 * jnp.abs(wave_third) <= tilt_limit * jnp.abs(wave_first)
    return inside.astype(jnp.float32)

def interpolate(stacked, kernels, grid_size):
    components = stacked.shape[0]
    kernels = kernels.astype(jnp.float32)
    along_first = jnp.einsum('ax,cxm->cam', kernels[0], stacked.astype(jnp.float32), precision=lax.Precision.HIGHEST).astype(jnp.bfloat16)
    along_first = along_first.reshape(components, grid_size, grid_size, grid_size)
    along_second = jnp.einsum('by,cayz->cabz', kernels[1], along_first.astype(jnp.float32), precision=lax.Precision.HIGHEST).astype(jnp.bfloat16)
    along_third = jnp.einsum('dz,cabz->cabd', kernels[2], along_second.astype(jnp.float32), precision=lax.Precision.HIGHEST)
    return along_third.reshape(components, grid_size, grid_size * grid_size)

def reference(particles, orient_bin, tilt_slope, interp_table):
    grid_size = GRID
    half_labels = (jnp.arange(PARTICLES, dtype=jnp.int32) // (PARTICLES // 2)).astype(jnp.int32)

    def insert_one(partial_value, inputs):
        volume_data, bin_row, tilt_limits, half_label = inputs
        weight = wedge_mask(tilt_limits, grid_size)
        stacked = jnp.stack([volume_data[0] * weight, volume_data[1] * weight, weight]).astype(jnp.bfloat16)
        kernels = interp_table[bin_row]
        inserted = interpolate(stacked, kernels, grid_size)
        partial_value = partial_value.at[half_label].add(inserted)
        return (partial_value, None)
    partial_value = jnp.zeros((2, 3, grid_size, grid_size * grid_size), jnp.float32)
    partial_value, unused_out = lax.scan(insert_one, partial_value, (particles, orient_bin, tilt_slope, half_labels))
    half_maps = partial_value[:, :2] / (partial_value[:, 2:3] + 1.0)
    centre = grid_size // 2
    wave_first = (jnp.arange(grid_size, dtype=jnp.int32) - centre)[:, None]
    plane_index = jnp.arange(grid_size * grid_size, dtype=jnp.int32)[None, :]
    wave_second = plane_index // grid_size - centre
    wave_third = plane_index % grid_size - centre
    radius_sq = (wave_first * wave_first + wave_second * wave_second + wave_third * wave_third).reshape(-1)
    bounds = jnp.arange(4, centre, dtype=jnp.int32)
    shell_index = lax.optimization_barrier(jnp.sum((radius_sq[:, None] >= (bounds * bounds)[None, :]).astype(jnp.int32), axis=1)).astype(jnp.int32)
    shell_index = jnp.where(radius_sq < centre * centre, shell_index, SHELLS).astype(jnp.int32)
    map_first = half_maps[0]
    map_second = half_maps[1]
    cross_term = (map_first[0] * map_second[0] + map_first[1] * map_second[1]).reshape(-1)
    power_first = (map_first[0] * map_first[0] + map_first[1] * map_first[1]).reshape(-1)
    power_second = (map_second[0] * map_second[0] + map_second[1] * map_second[1]).reshape(-1)

    def shell_sum(values):
        return jax.ops.segment_sum(values, shell_index, num_segments=SHELLS + 1)[:SHELLS]
    cross_sum = shell_sum(cross_term)
    first_sum = shell_sum(power_first)
    second_sum = shell_sum(power_second)
    counts = shell_sum(jnp.ones_like(cross_term))
    shell_power = jnp.stack([first_sum, second_sum]) / counts[None, :]
    correlation = cross_sum / jnp.sqrt(first_sum * second_sum + 1e-06)
    shell_correlation = jnp.stack([correlation, correlation])
    return (half_maps, shell_power, shell_correlation)
```

```python
import functools

import jax
import jax.numpy as jnp
import numpy as np
from jax import lax
from jax.experimental import pallas as pl
from jax.experimental.pallas import tpu as pltpu
from jax.sharding import PartitionSpec as P

F32 = jnp.float32
BF16 = jnp.bfloat16
LANES = 128
MESH = pl.DeviceIdType.MESH


def dot_nt(left, right):
    return lax.dot_general(left, right, (((1,), (1,)), ((), ())), preferred_element_type=F32)


def dot_nn(left, right):
    return lax.dot_general(left, right, (((1,), (0,)), ((), ())), preferred_element_type=F32)


def block_diagonal(block, copies):
    zero = jnp.zeros_like(block)
    rows = [
        jnp.concatenate([block if i == j else zero for j in range(copies)], axis=1)
        for i in range(copies)
    ]
    return jnp.concatenate(rows, axis=0)


def wedge_mask(limit_same, limit_other, grid, lanes):
    centre = grid // 2
    first = lax.broadcasted_iota(jnp.int32, (grid, lanes), 0) - centre
    third = lax.broadcasted_iota(jnp.int32, (grid, lanes), 1) % grid - centre
    limit = jnp.where(first * third >= 0, limit_same, limit_other)
    inside = 16 * jnp.abs(third) <= limit * jnp.abs(first)
    return jnp.where(inside, 1.0, 0.0).astype(BF16)


def shell_counts(grid):
    centre = grid // 2
    wave = np.arange(grid) - centre
    square = wave * wave
    radius = square[:, None, None] + square[None, :, None] + square[None, None, :]
    shell = np.sum([radius >= k * k for k in range(4, centre)], axis=0)
    return np.bincount(shell[radius < centre * centre], minlength=centre - 3)


def kernel(
    dims,
    bins_ref, tilt_ref, part_ref, table_ref, counts_ref,
    maps_ref, power_ref, corr_ref,
    stage_a, stage_b, sums, rows_in, cols_in, other_map,
    numbers, numbers_in, numbers_s, slab_first, slab_second, weight,
    stats, stats_in, total,
    send_row, recv_row, send_col, recv_col, send_num, recv_num, copy_num,
    send_stat, recv_stat, send_half, recv_half,
):
    grid, particles, R, C, pitch = dims
    N = R * C
    rl, bl = grid // R, grid // C
    cl = bl * grid
    phases = R.bit_length() - 1
    half, row, col = lax.axis_index("half"), lax.axis_index("row"), lax.axis_index("col")
    me = row * C + col

    def peer_id(step):
        peer = (me + step) % N
        return {"row": peer // C, "col": peer % C}

    def power_of(phase):
        low, high = 2 ** (phase % phases), 2 ** ((phase + 1) % phases)
        return low + half * (high - low)

    def row_partner(phase):
        weight_of = power_of(phase)
        bit = (row // weight_of) % 2
        return {"row": row + (1 - 2 * bit) * weight_of}

    def slab_of(index):
        slab = row
        for phase in range(phases):
            if (index >> (phases - 1 - phase)) & 1:
                weight_of = power_of(phase)
                bit = (row // weight_of) % 2
                slab = slab + (1 - 2 * bit) * weight_of
        return slab

    barrier = pltpu.get_barrier_semaphore()
    for step in range(1, N):
        pl.semaphore_signal(barrier, inc=1, device_id=peer_id(step), device_id_type=MESH)
    pl.semaphore_signal(barrier, inc=1, device_id={"half": 1 - half}, device_id_type=MESH)

    lane = lax.broadcasted_iota(jnp.int32, (1, LANES), 1)
    packed = jnp.zeros((1, LANES), jnp.int32)
    for p in range(particles):
        for i, value in enumerate((bins_ref[p], tilt_ref[p, 0], tilt_ref[p, 1])):
            packed = jnp.where(lane == 3 * p + i, value, packed)
    numbers[0] = packed
    numbers_in[me] = packed

    tiles = 4
    width = tiles * LANES
    seconds = width // grid

    for p in range(particles):
        bin_row = bins_ref[p]
        first = table_ref[bin_row, 0].astype(F32)
        second = table_ref[bin_row, 1].astype(F32)
        for r in range(R):
            slab_first[p, r] = first[r * rl:(r + 1) * rl]
        for q in range(C):
            slab_second[p, q] = second[q * bl:(q + 1) * bl]
        first = jnp.concatenate([slab_first[p, slab_of(j)] for j in range(R)], axis=0).astype(BF16)
        second = jnp.concatenate(
            [slab_second[p, (col + 1 + k) % C] for k in range(C)], axis=0
        ).astype(BF16)
        first = block_diagonal(first, 2)
        mask = wedge_mask(tilt_ref[p, 0], tilt_ref[p, 1], grid, LANES)
        mask = jnp.concatenate([mask] * tiles, axis=1)
        mask = jnp.concatenate([mask, mask], axis=0)

        def along_first(step, carry):
            span = pl.ds(pl.multiple_of(step * width, width), width)
            block = jnp.concatenate([part_ref[p, 0, :, span], part_ref[p, 1, :, span]], axis=0)
            result = dot_nt((block * mask).T, first)
            for i in range(seconds):
                at = pl.multiple_of((step * seconds + i) * pitch, 8)
                stage_a[pl.ds(at, grid), :] = result[i * grid:(i + 1) * grid]
            return carry

        lax.fori_loop(0, grid * grid // width, along_first, 0, unroll=2)

        for z in range(0, grid, 2):
            block = jnp.concatenate(
                [stage_a[pl.ds(z + i, grid, stride=pitch), :] for i in range(2)], axis=1
            ).astype(BF16)
            result = dot_nn(second, block)
            for i in range(2):
                stage_b[p, pl.ds((z + i) * pitch, grid), :] = result[:, i * LANES:(i + 1) * LANES]

    pl.semaphore_wait(barrier, N)

    num_copies = [
        pltpu.make_async_remote_copy(
            src_ref=numbers.at[0], dst_ref=numbers_in.at[me],
            send_sem=send_num.at[step - 1], recv_sem=recv_num.at[step - 1],
            device_id=peer_id(step), device_id_type=MESH,
        )
        for step in range(1, N)
    ]
    for copy in num_copies:
        copy.start()

    def row_copy(phase, k):
        keep = R >> (phase + 1)
        return pltpu.make_async_remote_copy(
            src_ref=sums.at[k, pl.ds(keep, keep)],
            dst_ref=rows_in.at[k, pl.ds(keep, keep)],
            send_sem=send_row.at[phase, k], recv_sem=recv_row.at[phase, k],
            device_id=row_partner(phase), device_id_type=MESH,
        )

    def col_copy(k):
        return pltpu.make_async_remote_copy(
            src_ref=sums.at[k, 0], dst_ref=cols_in.at[k],
            send_sem=send_col.at[k], recv_sem=recv_col.at[k],
            device_id={"col": (col + 1 + k) % C}, device_id_type=MESH,
        )

    third = jnp.concatenate(
        [block_diagonal(table_ref[bins_ref[p], 2], 2) for p in range(particles)], axis=1
    )
    for k in range(C):
        for pair in range(bl // 2):
            at = k * bl + 2 * pair
            block = jnp.concatenate(
                [
                    stage_b[p, pl.ds(at + i, grid, stride=pitch), :]
                    for p in range(particles)
                    for i in range(2)
                ],
                axis=0,
            ).astype(BF16)
            result = dot_nt(block.T, third)
            for j in range(R):
                for c in range(2):
                    sums[k, j, c, :, pair * LANES:(pair + 1) * LANES] = result[
                        c * grid + j * rl:c * grid + (j + 1) * rl
                    ]
        row_copy(0, k).start()

    for copy in num_copies:
        copy.wait_recv()
    local = pltpu.make_async_copy(numbers_in, numbers_s, copy_num)
    local.start()
    local.wait()
    weight[...] = jnp.zeros_like(weight)
    ones = jnp.ones((grid, grid), BF16)

    def add_weight(n, carry):
        firsts, seconds_, thirds = [], [], []
        for p in range(particles):
            bin_row = numbers_s[n, 0, 3 * p]
            mask = wedge_mask(numbers_s[n, 0, 3 * p + 1], numbers_s[n, 0, 3 * p + 2], grid, grid)
            first = dot_nn(table_ref[bin_row, 0], mask)
            second = dot_nn(table_ref[bin_row, 1], ones)
            for r in range(R):
                slab_first[p, r] = first[r * rl:(r + 1) * rl]
            for q in range(C):
                slab_second[p, q] = second[q * bl:(q + 1) * bl]
            firsts.append(slab_first[p, row])
            seconds_.append(slab_second[p, col])
            thirds.append(table_ref[bin_row, 2])
        first = jnp.concatenate(firsts, axis=1).astype(BF16).astype(F32)
        second = jnp.concatenate(seconds_, axis=1)
        third_ = jnp.concatenate(thirds, axis=1)
        block = jnp.concatenate([first * second[b:b + 1] for b in range(bl)], axis=0)
        weight[...] += dot_nt(block.astype(BF16), third_)
        return carry

    share = N // C
    for step in range(C + phases):
        if step < C:
            lax.fori_loop(step * share, (step + 1) * share, add_weight, 0)
        for phase in range(phases):
            k = step - phase
            if 0 <= k < C:
                keep = R >> (phase + 1)
                row_copy(phase, k).wait_recv()
                sums[k, :keep] = sums[k, :keep] + rows_in[k, keep:2 * keep]
                if phase + 1 < phases:
                    row_copy(phase + 1, k).start()
                elif k < C - 1:
                    col_copy(k).start()

    for k in range(C - 1):
        col_copy(k).wait_recv()
    for pair in range(bl // 2):
        span = slice(pair * LANES, (pair + 1) * LANES)
        low = 2 * pair * rl
        below = jnp.concatenate(
            [weight[low:low + rl], weight[low + rl:low + 2 * rl]], axis=1
        ) + 1.0
        for c in range(2):
            above = sums[C - 1, 0, c, :, span]
            for k in range(C - 1):
                above = above + cols_in[k, c, :, span]
            maps_ref[0, c, :, span] = above / below

    half_copy = pltpu.make_async_remote_copy(
        src_ref=maps_ref.at[0], dst_ref=other_map, send_sem=send_half, recv_sem=recv_half,
        device_id={"half": 1 - half}, device_id_type=MESH,
    )
    half_copy.start()
    for k in range(C):
        for phase in range(phases):
            row_copy(phase, k).wait_send()
    for k in range(C - 1):
        col_copy(k).wait_send()
    for copy in num_copies:
        copy.wait_send()
    half_copy.wait()

    centre = grid // 2
    shells = centre - 3
    tile_rows = lax.broadcasted_iota(jnp.int32, (rl, LANES), 0)
    tile_lanes = lax.broadcasted_iota(jnp.int32, (rl, LANES), 1)
    wave_first = row * rl + tile_rows - centre
    wave_third = tile_lanes % grid - centre
    on_first = (1 - half).astype(F32)
    on_second = half.astype(F32)
    fixed = wave_first * wave_first + wave_third * wave_third
    radius, products = [], []
    for pair in range(bl // 2):
        span = slice(pair * LANES, (pair + 1) * LANES)
        wave_second = col * bl + 2 * pair + tile_lanes // grid - centre
        radius.append(fixed + wave_second * wave_second)
        mine = [maps_ref[0, c, :, span] for c in range(2)]
        theirs = [other_map[c, :, span] for c in range(2)]
        own = mine[0] * mine[0] + mine[1] * mine[1]
        far = theirs[0] * theirs[0] + theirs[1] * theirs[1]
        products.append((
            mine[0] * theirs[0] + mine[1] * theirs[1],
            on_first * own + on_second * far,
            on_first * far + on_second * own,
        ))
    stats[...] = jnp.zeros_like(stats)
    for s in range(shells):
        least = (s + 3) * (s + 3) if s else 0
        beyond = (s + 4) * (s + 4)
        parts = [jnp.zeros((rl, LANES), F32) for _ in range(3)]
        for r2, values in zip(radius, products):
            inside = (r2 >= least) & (r2 < beyond)
            parts = [part + jnp.where(inside, value, 0.0) for part, value in zip(parts, values)]
        for i in range(3):
            stats[i * 32 + s:i * 32 + s + 1, :] = jnp.sum(parts[i], axis=0, keepdims=True)
    mine = jnp.sum(stats[...].T, axis=0, keepdims=True)
    total[0] = mine
    stats_in[me] = mine
    stat_copies = [
        pltpu.make_async_remote_copy(
            src_ref=total.at[0], dst_ref=stats_in.at[me],
            send_sem=send_stat.at[step - 1], recv_sem=recv_stat.at[step - 1],
            device_id=peer_id(step), device_id_type=MESH,
        )
        for step in range(1, N)
    ]
    for copy in stat_copies:
        copy.start()
    for copy in stat_copies:
        copy.wait()
    spectra = stats_in[0]
    for n in range(1, N):
        spectra = spectra + stats_in[n]
    cross = spectra[:, 0:shells]
    power_first = spectra[:, 32:32 + shells]
    power_second = spectra[:, 64:64 + shells]
    power_ref[0:1, :] = power_first / counts_ref[...]
    power_ref[1:2, :] = power_second / counts_ref[...]
    corr_ref[...] = cross / jnp.sqrt(power_first * power_second + 1e-6)


def solution(mesh):
    R, C = mesh.shape["row"], mesh.shape["col"]
    N = R * C

    def local(particles, orient_bin, tilt_slope, interp_table):
        count, _, grid, plane = particles.shape
        rl, cl, bl = grid // R, plane // C, grid // C
        shells = grid // 2 - 3
        phases = R.bit_length() - 1
        pitch = grid + 8
        counts = jnp.asarray(shell_counts(grid)[None], F32)
        vmem, smem = pl.BlockSpec(memory_space=pltpu.VMEM), pl.BlockSpec(memory_space=pltpu.SMEM)
        dma = pltpu.SemaphoreType.DMA
        return pl.pallas_call(
            functools.partial(kernel, (grid, count, R, C, pitch)),
            out_shape=(
                jax.ShapeDtypeStruct((1, 2, rl, cl), F32),
                jax.ShapeDtypeStruct((2, shells), F32),
                jax.ShapeDtypeStruct((1, shells), F32),
            ),
            in_specs=[smem, smem, vmem, vmem, vmem],
            out_specs=(vmem, vmem, vmem),
            scratch_shapes=[
                pltpu.VMEM((grid * pitch, LANES), F32),
                pltpu.VMEM((count, grid * pitch, LANES), F32),
                pltpu.VMEM((C, R, 2, rl, cl), F32),
                pltpu.VMEM((C, R, 2, rl, cl), F32),
                pltpu.VMEM((C - 1, 2, rl, cl), F32),
                pltpu.VMEM((2, rl, cl), F32),
                pltpu.VMEM((1, 1, LANES), jnp.int32),
                pltpu.VMEM((N, 1, LANES), jnp.int32),
                pltpu.SMEM((N, 1, LANES), jnp.int32),
                pltpu.VMEM((count, R, rl, grid), F32),
                pltpu.VMEM((count, C, bl, grid), F32),
                pltpu.VMEM((bl * rl, grid), F32),
                pltpu.VMEM((LANES, LANES), F32),
                pltpu.VMEM((N, 1, LANES), F32),
                pltpu.VMEM((1, 1, LANES), F32),
                dma((phases, C)), dma((phases, C)),
                dma((C - 1,)), dma((C - 1,)),
                dma((N - 1,)), dma((N - 1,)), dma,
                dma((N - 1,)), dma((N - 1,)),
                dma, dma,
            ],
            compiler_params=pltpu.CompilerParams(
                collective_id=0, has_side_effects=True, vmem_limit_bytes=56 * 1024 * 1024
            ),
        )(orient_bin, tilt_slope, particles, interp_table, counts)

    placed = (
        P(("half", "row", "col"), None, None, None),
        P(("half", "row", "col")),
        P(("half", "row", "col"), None),
        P(),
    )
    return jax.shard_map(
        local,
        mesh=mesh,
        in_specs=placed,
        out_specs=(P("half", None, "row", "col"), P(), P("half", None)),
        check_vma=False,
    )
```

```python
import functools

import jax
import jax.numpy as jnp
import numpy as np
from jax import lax
from jax.experimental import pallas as pl
from jax.experimental.pallas import tpu as pltpu
from jax.sharding import PartitionSpec as P

F32 = jnp.float32
BF16 = jnp.bfloat16
LANES = 128
MESH = pl.DeviceIdType.MESH


def dot_nt(left, right):
    return lax.dot_general(left, right, (((1,), (1,)), ((), ())), preferred_element_type=F32)


def dot_nn(left, right):
    return lax.dot_general(left, right, (((1,), (0,)), ((), ())), preferred_element_type=F32)


def block_diagonal(block, copies):
    zero = jnp.zeros_like(block)
    rows = [
        jnp.concatenate([block if i == j else zero for j in range(copies)], axis=1)
        for i in range(copies)
    ]
    return jnp.concatenate(rows, axis=0)


def wedge_mask(limit_same, limit_other, grid, lanes):
    centre = grid // 2
    first = lax.broadcasted_iota(jnp.int32, (grid, lanes), 0) - centre
    third = lax.broadcasted_iota(jnp.int32, (grid, lanes), 1) % grid - centre
    limit = jnp.where(first * third >= 0, limit_same, limit_other)
    inside = 16 * jnp.abs(third) <= limit * jnp.abs(first)
    return jnp.where(inside, 1.0, 0.0).astype(BF16)


def shell_counts(grid):
    centre = grid // 2
    wave = np.arange(grid) - centre
    square = wave * wave
    radius = square[:, None, None] + square[None, :, None] + square[None, None, :]
    shell = np.sum([radius >= k * k for k in range(4, centre)], axis=0)
    return np.bincount(shell[radius < centre * centre], minlength=centre - 3)


def kernel(
    dims,
    bins_ref, tilt_ref, part_hbm, table_hbm,
    maps_ref, spectra_ref,
    part_ref, table_ref, stage_a, stage_b, sums, rows_in, cols_in, other_map,
    numbers, numbers_in, numbers_s, slab_first, slab_second, weight,
    stats, stats_in, total,
    send_row, recv_row, send_col, recv_col, send_num, recv_num, copy_num,
    send_stat, recv_stat, send_half, recv_half, load_part, load_table,
):
    grid, particles, R, C, pitch = dims
    N = R * C
    rl, bl = grid // R, grid // C
    cl = bl * grid
    phases = R.bit_length() - 1
    half, row, col = lax.axis_index("half"), lax.axis_index("row"), lax.axis_index("col")
    me = row * C + col

    def peer_id(step):
        peer = (me + step) % N
        return {"row": peer // C, "col": peer % C}

    def power_of(phase):
        low, high = 2 ** (phase % phases), 2 ** ((phase + 1) % phases)
        return low + half * (high - low)

    def row_partner(phase):
        weight_of = power_of(phase)
        bit = (row // weight_of) % 2
        return {"row": row + (1 - 2 * bit) * weight_of}

    def slab_of(index):
        slab = row
        for phase in range(phases):
            if (index >> (phases - 1 - phase)) & 1:
                weight_of = power_of(phase)
                bit = (row // weight_of) % 2
                slab = slab + (1 - 2 * bit) * weight_of
        return slab

    table_load = pltpu.make_async_copy(table_hbm, table_ref, load_table)
    table_load.start()
    part_loads = [
        pltpu.make_async_copy(part_hbm.at[p], part_ref.at[p], load_part.at[p])
        for p in range(particles)
    ]
    for copy in part_loads:
        copy.start()

    barrier = pltpu.get_barrier_semaphore()
    for step in range(1, N):
        pl.semaphore_signal(barrier, inc=1, device_id=peer_id(step), device_id_type=MESH)
    pl.semaphore_signal(barrier, inc=1, device_id={"half": 1 - half}, device_id_type=MESH)

    lane = lax.broadcasted_iota(jnp.int32, (1, LANES), 1)
    packed = jnp.zeros((1, LANES), jnp.int32)
    for p in range(particles):
        for i, value in enumerate((bins_ref[p], tilt_ref[p, 0], tilt_ref[p, 1])):
            packed = jnp.where(lane == 3 * p + i, value, packed)
    numbers[0] = packed
    numbers_in[me] = packed

    tiles = 4
    width = tiles * LANES
    seconds = width // grid

    table_load.wait()
    for p in range(particles):
        bin_row = bins_ref[p]
        first = table_ref[bin_row, 0].astype(F32)
        second = table_ref[bin_row, 1].astype(F32)
        for r in range(R):
            slab_first[p, r] = first[r * rl:(r + 1) * rl]
        for q in range(C):
            slab_second[p, q] = second[q * bl:(q + 1) * bl]
        first = jnp.concatenate([slab_first[p, slab_of(j)] for j in range(R)], axis=0).astype(BF16)
        second = jnp.concatenate(
            [slab_second[p, (col + 1 + k) % C] for k in range(C)], axis=0
        ).astype(BF16)
        first = block_diagonal(first, 2)
        mask = wedge_mask(tilt_ref[p, 0], tilt_ref[p, 1], grid, LANES)
        mask = jnp.concatenate([mask] * tiles, axis=1)
        mask = jnp.concatenate([mask, mask], axis=0)

        def along_first(step, carry):
            span = pl.ds(pl.multiple_of(step * width, width), width)
            block = jnp.concatenate([part_ref[p, 0, :, span], part_ref[p, 1, :, span]], axis=0)
            result = dot_nt((block * mask).T, first)
            for i in range(seconds):
                at = pl.multiple_of((step * seconds + i) * pitch, 8)
                stage_a[pl.ds(at, grid), :] = result[i * grid:(i + 1) * grid]
            return carry

        part_loads[p].wait()
        lax.fori_loop(0, grid * grid // width, along_first, 0, unroll=2)

        for z in range(0, grid, 2):
            block = jnp.concatenate(
                [stage_a[pl.ds(z + i, grid, stride=pitch), :] for i in range(2)], axis=1
            ).astype(BF16)
            result = dot_nn(second, block)
            for i in range(2):
                stage_b[p, pl.ds((z + i) * pitch, grid), :] = result[:, i * LANES:(i + 1) * LANES]

    pl.semaphore_wait(barrier, N)

    num_copies = [
        pltpu.make_async_remote_copy(
            src_ref=numbers.at[0], dst_ref=numbers_in.at[me],
            send_sem=send_num.at[step - 1], recv_sem=recv_num.at[step - 1],
            device_id=peer_id(step), device_id_type=MESH,
        )
        for step in range(1, N)
    ]
    for copy in num_copies:
        copy.start()

    def row_copy(phase, k):
        keep = R >> (phase + 1)
        return pltpu.make_async_remote_copy(
            src_ref=sums.at[k, pl.ds(keep, keep)],
            dst_ref=rows_in.at[k, pl.ds(keep, keep)],
            send_sem=send_row.at[phase, k], recv_sem=recv_row.at[phase, k],
            device_id=row_partner(phase), device_id_type=MESH,
        )

    def col_copy(k):
        return pltpu.make_async_remote_copy(
            src_ref=sums.at[k, 0], dst_ref=cols_in.at[k],
            send_sem=send_col.at[k], recv_sem=recv_col.at[k],
            device_id={"col": (col + 1 + k) % C}, device_id_type=MESH,
        )

    third = jnp.concatenate(
        [block_diagonal(table_ref[bins_ref[p], 2], 2) for p in range(particles)], axis=1
    )
    for k in range(C):
        for pair in range(bl // 2):
            at = k * bl + 2 * pair
            block = jnp.concatenate(
                [
                    stage_b[p, pl.ds(at + i, grid, stride=pitch), :]
                    for p in range(particles)
                    for i in range(2)
                ],
                axis=0,
            ).astype(BF16)
            result = dot_nt(block.T, third)
            for j in range(R):
                for c in range(2):
                    sums[k, j, c, :, pair * LANES:(pair + 1) * LANES] = result[
                        c * grid + j * rl:c * grid + (j + 1) * rl
                    ]
        row_copy(0, k).start()

    for copy in num_copies:
        copy.wait_recv()
    local = pltpu.make_async_copy(numbers_in, numbers_s, copy_num)
    local.start()
    local.wait()
    weight[...] = jnp.zeros_like(weight)
    ones = jnp.ones((grid, grid), BF16)

    def add_weight(n, carry):
        firsts, seconds_, thirds = [], [], []
        for p in range(particles):
            bin_row = numbers_s[n, 0, 3 * p]
            mask = wedge_mask(numbers_s[n, 0, 3 * p + 1], numbers_s[n, 0, 3 * p + 2], grid, grid)
            first = dot_nn(table_ref[bin_row, 0], mask)
            second = dot_nn(table_ref[bin_row, 1], ones)
            for r in range(R):
                slab_first[p, r] = first[r * rl:(r + 1) * rl]
            for q in range(C):
                slab_second[p, q] = second[q * bl:(q + 1) * bl]
            firsts.append(slab_first[p, row])
            seconds_.append(slab_second[p, col])
            thirds.append(table_ref[bin_row, 2])
        first = jnp.concatenate(firsts, axis=1).astype(BF16).astype(F32)
        second = jnp.concatenate(seconds_, axis=1)
        third_ = jnp.concatenate(thirds, axis=1)
        block = jnp.concatenate([first * second[b:b + 1] for b in range(bl)], axis=0)
        weight[...] += dot_nt(block.astype(BF16), third_)
        return carry

    share = N // C
    for step in range(C + phases):
        if step < C:
            lax.fori_loop(step * share, (step + 1) * share, add_weight, 0)
        for phase in range(phases):
            k = step - phase
            if 0 <= k < C:
                keep = R >> (phase + 1)
                row_copy(phase, k).wait_recv()
                sums[k, :keep] = sums[k, :keep] + rows_in[k, keep:2 * keep]
                if phase + 1 < phases:
                    row_copy(phase + 1, k).start()
                elif k < C - 1:
                    col_copy(k).start()

    for k in range(C - 1):
        col_copy(k).wait_recv()
    for pair in range(bl // 2):
        span = slice(pair * LANES, (pair + 1) * LANES)
        low = 2 * pair * rl
        below = jnp.concatenate(
            [weight[low:low + rl], weight[low + rl:low + 2 * rl]], axis=1
        ) + 1.0
        for c in range(2):
            above = sums[C - 1, 0, c, :, span]
            for k in range(C - 1):
                above = above + cols_in[k, c, :, span]
            maps_ref[0, c, :, span] = above / below

    half_copy = pltpu.make_async_remote_copy(
        src_ref=maps_ref.at[0], dst_ref=other_map, send_sem=send_half, recv_sem=recv_half,
        device_id={"half": 1 - half}, device_id_type=MESH,
    )
    half_copy.start()
    for k in range(C):
        for phase in range(phases):
            row_copy(phase, k).wait_send()
    for k in range(C - 1):
        col_copy(k).wait_send()
    for copy in num_copies:
        copy.wait_send()
    half_copy.wait()

    centre = grid // 2
    shells = centre - 3
    tile_rows = lax.broadcasted_iota(jnp.int32, (rl, LANES), 0)
    tile_lanes = lax.broadcasted_iota(jnp.int32, (rl, LANES), 1)
    wave_first = row * rl + tile_rows - centre
    wave_third = tile_lanes % grid - centre
    on_first = (1 - half).astype(F32)
    on_second = half.astype(F32)
    fixed = wave_first * wave_first + wave_third * wave_third
    radius, products = [], []
    for pair in range(bl // 2):
        span = slice(pair * LANES, (pair + 1) * LANES)
        wave_second = col * bl + 2 * pair + tile_lanes // grid - centre
        radius.append(fixed + wave_second * wave_second)
        mine = [maps_ref[0, c, :, span] for c in range(2)]
        theirs = [other_map[c, :, span] for c in range(2)]
        own = mine[0] * mine[0] + mine[1] * mine[1]
        far = theirs[0] * theirs[0] + theirs[1] * theirs[1]
        products.append((
            mine[0] * theirs[0] + mine[1] * theirs[1],
            on_first * own + on_second * far,
            on_first * far + on_second * own,
        ))
    stats[...] = jnp.zeros_like(stats)
    for s in range(shells):
        least = (s + 3) * (s + 3) if s else 0
        beyond = (s + 4) * (s + 4)
        parts = [jnp.zeros((rl, LANES), F32) for _ in range(3)]
        for r2, values in zip(radius, products):
            inside = (r2 >= least) & (r2 < beyond)
            parts = [part + jnp.where(inside, value, 0.0) for part, value in zip(parts, values)]
        for i in range(3):
            stats[i * 32 + s:i * 32 + s + 1, :] = jnp.sum(parts[i], axis=0, keepdims=True)
    mine = jnp.sum(stats[...].T, axis=0, keepdims=True)
    total[0] = mine
    stats_in[me] = mine
    stat_copies = [
        pltpu.make_async_remote_copy(
            src_ref=total.at[0], dst_ref=stats_in.at[me],
            send_sem=send_stat.at[step - 1], recv_sem=recv_stat.at[step - 1],
            device_id=peer_id(step), device_id_type=MESH,
        )
        for step in range(1, N)
    ]
    for copy in stat_copies:
        copy.start()
    for copy in stat_copies:
        copy.wait()
    spectra = stats_in[0]
    for n in range(1, N):
        spectra = spectra + stats_in[n]
    spectra_ref[...] = spectra


def finish(shells, maps_in_ref, spectra_ref, counts_ref, maps_ref, power_ref, corr_ref):
    maps_ref[...] = maps_in_ref[...]
    spectra = spectra_ref[...]
    cross = spectra[:, 0:shells]
    power_first = spectra[:, 32:32 + shells]
    power_second = spectra[:, 64:64 + shells]
    power_ref[0:1, :] = power_first / counts_ref[...]
    power_ref[1:2, :] = power_second / counts_ref[...]
    corr_ref[...] = cross / jnp.sqrt(power_first * power_second + 1e-6)


def solution(mesh):
    R, C = mesh.shape["row"], mesh.shape["col"]
    N = R * C

    def local(particles, orient_bin, tilt_slope, interp_table):
        count, _, grid, plane = particles.shape
        rl, cl, bl = grid // R, plane // C, grid // C
        shells = grid // 2 - 3
        phases = R.bit_length() - 1
        pitch = grid + 8
        counts = jnp.asarray(shell_counts(grid)[None], F32)
        vmem, smem = pl.BlockSpec(memory_space=pltpu.VMEM), pl.BlockSpec(memory_space=pltpu.SMEM)
        anywhere = pl.BlockSpec(memory_space=pl.ANY)
        dma = pltpu.SemaphoreType.DMA
        maps, spectra = pl.pallas_call(
            functools.partial(kernel, (grid, count, R, C, pitch)),
            out_shape=(
                jax.ShapeDtypeStruct((1, 2, rl, cl), F32),
                jax.ShapeDtypeStruct((1, LANES), F32),
            ),
            in_specs=[smem, smem, anywhere, anywhere],
            out_specs=(vmem, vmem),
            scratch_shapes=[
                pltpu.VMEM(particles.shape, particles.dtype),
                pltpu.VMEM(interp_table.shape, interp_table.dtype),
                pltpu.VMEM((grid * pitch, LANES), F32),
                pltpu.VMEM((count, grid * pitch, LANES), F32),
                pltpu.VMEM((C, R, 2, rl, cl), F32),
                pltpu.VMEM((C, R, 2, rl, cl), F32),
                pltpu.VMEM((C - 1, 2, rl, cl), F32),
                pltpu.VMEM((2, rl, cl), F32),
                pltpu.VMEM((1, 1, LANES), jnp.int32),
                pltpu.VMEM((N, 1, LANES), jnp.int32),
                pltpu.SMEM((N, 1, LANES), jnp.int32),
                pltpu.VMEM((count, R, rl, grid), F32),
                pltpu.VMEM((count, C, bl, grid), F32),
                pltpu.VMEM((bl * rl, grid), F32),
                pltpu.VMEM((LANES, LANES), F32),
                pltpu.VMEM((N, 1, LANES), F32),
                pltpu.VMEM((1, 1, LANES), F32),
                dma((phases, C)), dma((phases, C)),
                dma((C - 1,)), dma((C - 1,)),
                dma((N - 1,)), dma((N - 1,)), dma,
                dma((N - 1,)), dma((N - 1,)),
                dma, dma, dma((count,)), dma,
            ],
            compiler_params=pltpu.CompilerParams(
                collective_id=0, has_side_effects=True, vmem_limit_bytes=56 * 1024 * 1024
            ),
        )(orient_bin, tilt_slope, particles, interp_table)
        return pl.pallas_call(
            functools.partial(finish, shells),
            out_shape=(
                jax.ShapeDtypeStruct((1, 2, rl, cl), F32),
                jax.ShapeDtypeStruct((2, shells), F32),
                jax.ShapeDtypeStruct((1, shells), F32),
            ),
            in_specs=[vmem, vmem, vmem],
            out_specs=(vmem, vmem, vmem),
        )(maps, spectra, counts)

    placed = (
        P(("half", "row", "col"), None, None, None),
        P(("half", "row", "col")),
        P(("half", "row", "col"), None),
        P(),
    )
    return jax.shard_map(
        local,
        mesh=mesh,
        in_specs=placed,
        out_specs=(P("half", None, "row", "col"), P(), P("half", None)),
        check_vma=False,
    )
```

```python
import functools

import jax
import jax.numpy as jnp
import numpy as np
from jax import lax
from jax.experimental import pallas as pl
from jax.experimental.pallas import tpu as pltpu
from jax.sharding import PartitionSpec as P

F32 = jnp.float32
BF16 = jnp.bfloat16
LANES = 128
MESH = pl.DeviceIdType.MESH


def dot_nt(left, right):
    return lax.dot_general(left, right, (((1,), (1,)), ((), ())), preferred_element_type=F32)


def dot_nn(left, right):
    return lax.dot_general(left, right, (((1,), (0,)), ((), ())), preferred_element_type=F32)


def block_diagonal(block, copies):
    zero = jnp.zeros_like(block)
    rows = [
        jnp.concatenate([block if i == j else zero for j in range(copies)], axis=1)
        for i in range(copies)
    ]
    return jnp.concatenate(rows, axis=0)


def wedge_mask(limit_same, limit_other, grid, lanes):
    centre = grid // 2
    first = lax.broadcasted_iota(jnp.int32, (grid, lanes), 0) - centre
    third = lax.broadcasted_iota(jnp.int32, (grid, lanes), 1) % grid - centre
    limit = jnp.where(first * third >= 0, limit_same, limit_other)
    inside = 16 * jnp.abs(third) <= limit * jnp.abs(first)
    return jnp.where(inside, 1.0, 0.0).astype(BF16)


def shell_counts(grid):
    centre = grid // 2
    wave = np.arange(grid) - centre
    square = wave * wave
    radius = square[:, None, None] + square[None, :, None] + square[None, None, :]
    shell = np.sum([radius >= k * k for k in range(4, centre)], axis=0)
    return np.bincount(shell[radius < centre * centre], minlength=centre - 3)


def kernel(
    dims,
    bins_ref, tilt_ref, part_hbm, table_hbm,
    maps_ref, spectra_ref,
    part_ref, table_ref, stage_a, stage_b, sums, rows_in, cols_in, other_map,
    numbers, numbers_in, numbers_s, slab_first, slab_second, weight,
    stats, stats_in, total,
    send_row, recv_row, send_col, recv_col, send_num, recv_num, copy_num,
    send_stat, recv_stat, send_half, recv_half, load_part, load_table,
):
    grid, particles, R, C, pitch = dims
    N = R * C
    rl, bl = grid // R, grid // C
    cl = bl * grid
    phases = R.bit_length() - 1
    half, row, col = lax.axis_index("half"), lax.axis_index("row"), lax.axis_index("col")
    me = row * C + col

    def peer_id(step):
        peer = (me + step) % N
        return {"row": peer // C, "col": peer % C}

    def power_of(phase):
        low, high = 2 ** (phase % phases), 2 ** ((phase + 1) % phases)
        return low + half * (high - low)

    def row_partner(phase):
        weight_of = power_of(phase)
        bit = (row // weight_of) % 2
        return {"row": row + (1 - 2 * bit) * weight_of}

    def slab_of(index):
        slab = row
        for phase in range(phases):
            if (index >> (phases - 1 - phase)) & 1:
                weight_of = power_of(phase)
                bit = (row // weight_of) % 2
                slab = slab + (1 - 2 * bit) * weight_of
        return slab

    table_load = pltpu.make_async_copy(table_hbm, table_ref, load_table)
    table_load.start()
    part_loads = [
        pltpu.make_async_copy(part_hbm.at[p], part_ref.at[p], load_part.at[p])
        for p in range(particles)
    ]
    for copy in part_loads:
        copy.start()

    barrier = pltpu.get_barrier_semaphore()
    for step in range(1, N):
        pl.semaphore_signal(barrier, inc=1, device_id=peer_id(step), device_id_type=MESH)
    pl.semaphore_signal(barrier, inc=1, device_id={"half": 1 - half}, device_id_type=MESH)

    lane = lax.broadcasted_iota(jnp.int32, (1, LANES), 1)
    packed = jnp.zeros((1, LANES), jnp.int32)
    for p in range(particles):
        for i, value in enumerate((bins_ref[p], tilt_ref[p, 0], tilt_ref[p, 1])):
            packed = jnp.where(lane == 3 * p + i, value, packed)
    numbers[0] = packed
    numbers_in[me] = packed

    tiles = 4
    width = tiles * LANES
    seconds = width // grid

    table_load.wait()
    for p in range(particles):
        bin_row = bins_ref[p]
        first = table_ref[bin_row, 0].astype(F32)
        second = table_ref[bin_row, 1].astype(F32)
        for r in range(R):
            slab_first[p, r] = first[r * rl:(r + 1) * rl]
        for q in range(C):
            slab_second[p, q] = second[q * bl:(q + 1) * bl]
        first = jnp.concatenate([slab_first[p, slab_of(j)] for j in range(R)], axis=0).astype(BF16)
        second = jnp.concatenate(
            [slab_second[p, (col + 1 + k) % C] for k in range(C)], axis=0
        ).astype(BF16)
        first = block_diagonal(first, 2)
        mask = wedge_mask(tilt_ref[p, 0], tilt_ref[p, 1], grid, LANES)
        mask = jnp.concatenate([mask] * tiles, axis=1)
        mask = jnp.concatenate([mask, mask], axis=0)

        def along_first(step, carry):
            span = pl.ds(pl.multiple_of(step * width, width), width)
            block = jnp.concatenate([part_ref[p, 0, :, span], part_ref[p, 1, :, span]], axis=0)
            result = dot_nt((block * mask).T, first)
            for i in range(seconds):
                at = pl.multiple_of((step * seconds + i) * pitch, 8)
                stage_a[pl.ds(at, grid), :] = result[i * grid:(i + 1) * grid]
            return carry

        part_loads[p].wait()
        lax.fori_loop(0, grid * grid // width, along_first, 0, unroll=2)

        for z in range(0, grid, 2):
            block = jnp.concatenate(
                [stage_a[pl.ds(z + i, grid, stride=pitch), :] for i in range(2)], axis=1
            ).astype(BF16)
            result = dot_nn(second, block)
            for i in range(2):
                stage_b[p, pl.ds((z + i) * pitch, grid), :] = result[:, i * LANES:(i + 1) * LANES]

    pl.semaphore_wait(barrier, N)

    num_copies = [
        pltpu.make_async_remote_copy(
            src_ref=numbers.at[0], dst_ref=numbers_in.at[me],
            send_sem=send_num.at[step - 1], recv_sem=recv_num.at[step - 1],
            device_id=peer_id(step), device_id_type=MESH,
        )
        for step in range(1, N)
    ]
    for copy in num_copies:
        copy.start()

    def row_copy(phase, k):
        keep = R >> (phase + 1)
        return pltpu.make_async_remote_copy(
            src_ref=sums.at[k, pl.ds(keep, keep)],
            dst_ref=rows_in.at[k, pl.ds(keep, keep)],
            send_sem=send_row.at[phase, k], recv_sem=recv_row.at[phase, k],
            device_id=row_partner(phase), device_id_type=MESH,
        )

    def col_copy(k):
        return pltpu.make_async_remote_copy(
            src_ref=sums.at[k, 0], dst_ref=cols_in.at[k],
            send_sem=send_col.at[k], recv_sem=recv_col.at[k],
            device_id={"col": (col + 1 + k) % C}, device_id_type=MESH,
        )

    third = jnp.concatenate(
        [block_diagonal(table_ref[bins_ref[p], 2], 2) for p in range(particles)], axis=1
    )
    for k in range(C):
        for pair in range(bl // 2):
            at = k * bl + 2 * pair
            block = jnp.concatenate(
                [
                    stage_b[p, pl.ds(at + i, grid, stride=pitch), :]
                    for p in range(particles)
                    for i in range(2)
                ],
                axis=0,
            ).astype(BF16)
            result = dot_nt(block.T, third)
            for j in range(R):
                for c in range(2):
                    sums[k, j, c, :, pair * LANES:(pair + 1) * LANES] = result[
                        c * grid + j * rl:c * grid + (j + 1) * rl
                    ]
        row_copy(0, k).start()

    local = pltpu.make_async_copy(numbers_in, numbers_s, copy_num)
    weight[...] = jnp.zeros_like(weight)
    ones = jnp.ones((grid, grid), BF16)

    def add_weight(n, carry):
        firsts, seconds_, thirds = [], [], []
        for p in range(particles):
            bin_row = numbers_s[n, 0, 3 * p]
            mask = wedge_mask(numbers_s[n, 0, 3 * p + 1], numbers_s[n, 0, 3 * p + 2], grid, grid)
            first = dot_nn(table_ref[bin_row, 0], mask)
            second = dot_nn(table_ref[bin_row, 1], ones)
            for r in range(R):
                slab_first[p, r] = first[r * rl:(r + 1) * rl]
            for q in range(C):
                slab_second[p, q] = second[q * bl:(q + 1) * bl]
            firsts.append(slab_first[p, row])
            seconds_.append(slab_second[p, col])
            thirds.append(table_ref[bin_row, 2])
        first = jnp.concatenate(firsts, axis=1).astype(BF16).astype(F32)
        second = jnp.concatenate(seconds_, axis=1)
        third_ = jnp.concatenate(thirds, axis=1)
        block = jnp.concatenate([first * second[b:b + 1] for b in range(bl)], axis=0)
        weight[...] += dot_nt(block.astype(BF16), third_)
        return carry

    share = N // C
    for step in range(C + phases):
        for phase in range(phases):
            k = step - phase
            if 0 <= k < C:
                keep = R >> (phase + 1)
                row_copy(phase, k).wait_recv()
                sums[k, :keep] = sums[k, :keep] + rows_in[k, keep:2 * keep]
                if phase + 1 < phases:
                    row_copy(phase + 1, k).start()
                elif k < C - 1:
                    col_copy(k).start()
        if step == 0:
            for copy in num_copies:
                copy.wait_recv()
            local.start()
            local.wait()
        if step < C:
            lax.fori_loop(step * share, (step + 1) * share, add_weight, 0)

    for k in range(C - 1):
        col_copy(k).wait_recv()
    for pair in range(bl // 2):
        span = slice(pair * LANES, (pair + 1) * LANES)
        low = 2 * pair * rl
        below = jnp.concatenate(
            [weight[low:low + rl], weight[low + rl:low + 2 * rl]], axis=1
        ) + 1.0
        for c in range(2):
            above = sums[C - 1, 0, c, :, span]
            for k in range(C - 1):
                above = above + cols_in[k, c, :, span]
            maps_ref[0, c, :, span] = above / below

    half_copy = pltpu.make_async_remote_copy(
        src_ref=maps_ref.at[0], dst_ref=other_map, send_sem=send_half, recv_sem=recv_half,
        device_id={"half": 1 - half}, device_id_type=MESH,
    )
    half_copy.start()
    for k in range(C):
        for phase in range(phases):
            row_copy(phase, k).wait_send()
    for k in range(C - 1):
        col_copy(k).wait_send()
    for copy in num_copies:
        copy.wait_send()
    half_copy.wait()

    centre = grid // 2
    shells = centre - 3
    tile_rows = lax.broadcasted_iota(jnp.int32, (rl, LANES), 0)
    tile_lanes = lax.broadcasted_iota(jnp.int32, (rl, LANES), 1)
    wave_first = row * rl + tile_rows - centre
    wave_third = tile_lanes % grid - centre
    on_first = (1 - half).astype(F32)
    on_second = half.astype(F32)
    fixed = wave_first * wave_first + wave_third * wave_third
    radius, products = [], []
    for pair in range(bl // 2):
        span = slice(pair * LANES, (pair + 1) * LANES)
        wave_second = col * bl + 2 * pair + tile_lanes // grid - centre
        radius.append(fixed + wave_second * wave_second)
        mine = [maps_ref[0, c, :, span] for c in range(2)]
        theirs = [other_map[c, :, span] for c in range(2)]
        own = mine[0] * mine[0] + mine[1] * mine[1]
        far = theirs[0] * theirs[0] + theirs[1] * theirs[1]
        products.append((
            mine[0] * theirs[0] + mine[1] * theirs[1],
            on_first * own + on_second * far,
            on_first * far + on_second * own,
        ))
    stats[...] = jnp.zeros_like(stats)
    for s in range(shells):
        least = (s + 3) * (s + 3) if s else 0
        beyond = (s + 4) * (s + 4)
        parts = [jnp.zeros((rl, LANES), F32) for _ in range(3)]
        for r2, values in zip(radius, products):
            inside = (r2 >= least) & (r2 < beyond)
            parts = [part + jnp.where(inside, value, 0.0) for part, value in zip(parts, values)]
        for i in range(3):
            stats[i * 32 + s:i * 32 + s + 1, :] = jnp.sum(parts[i], axis=0, keepdims=True)
    mine = jnp.sum(stats[...].T, axis=0, keepdims=True)
    total[0] = mine
    stats_in[me] = mine
    stat_copies = [
        pltpu.make_async_remote_copy(
            src_ref=total.at[0], dst_ref=stats_in.at[me],
            send_sem=send_stat.at[step - 1], recv_sem=recv_stat.at[step - 1],
            device_id=peer_id(step), device_id_type=MESH,
        )
        for step in range(1, N)
    ]
    for copy in stat_copies:
        copy.start()
    for copy in stat_copies:
        copy.wait()
    spectra = stats_in[0]
    for n in range(1, N):
        spectra = spectra + stats_in[n]
    spectra_ref[...] = spectra


def finish(shells, maps_in_ref, spectra_ref, counts_ref, maps_ref, power_ref, corr_ref):
    maps_ref[...] = maps_in_ref[...]
    spectra = spectra_ref[...]
    cross = spectra[:, 0:shells]
    power_first = spectra[:, 32:32 + shells]
    power_second = spectra[:, 64:64 + shells]
    power_ref[0:1, :] = power_first / counts_ref[...]
    power_ref[1:2, :] = power_second / counts_ref[...]
    corr_ref[...] = cross / jnp.sqrt(power_first * power_second + 1e-6)


def solution(mesh):
    R, C = mesh.shape["row"], mesh.shape["col"]
    N = R * C

    def local(particles, orient_bin, tilt_slope, interp_table):
        count, _, grid, plane = particles.shape
        rl, cl, bl = grid // R, plane // C, grid // C
        shells = grid // 2 - 3
        phases = R.bit_length() - 1
        pitch = grid + 8
        counts = jnp.asarray(shell_counts(grid)[None], F32)
        vmem, smem = pl.BlockSpec(memory_space=pltpu.VMEM), pl.BlockSpec(memory_space=pltpu.SMEM)
        anywhere = pl.BlockSpec(memory_space=pl.ANY)
        dma = pltpu.SemaphoreType.DMA
        maps, spectra = pl.pallas_call(
            functools.partial(kernel, (grid, count, R, C, pitch)),
            out_shape=(
                jax.ShapeDtypeStruct((1, 2, rl, cl), F32),
                jax.ShapeDtypeStruct((1, LANES), F32),
            ),
            in_specs=[smem, smem, anywhere, anywhere],
            out_specs=(vmem, vmem),
            scratch_shapes=[
                pltpu.VMEM(particles.shape, particles.dtype),
                pltpu.VMEM(interp_table.shape, interp_table.dtype),
                pltpu.VMEM((grid * pitch, LANES), F32),
                pltpu.VMEM((count, grid * pitch, LANES), F32),
                pltpu.VMEM((C, R, 2, rl, cl), F32),
                pltpu.VMEM((C, R, 2, rl, cl), F32),
                pltpu.VMEM((C - 1, 2, rl, cl), F32),
                pltpu.VMEM((2, rl, cl), F32),
                pltpu.VMEM((1, 1, LANES), jnp.int32),
                pltpu.VMEM((N, 1, LANES), jnp.int32),
                pltpu.SMEM((N, 1, LANES), jnp.int32),
                pltpu.VMEM((count, R, rl, grid), F32),
                pltpu.VMEM((count, C, bl, grid), F32),
                pltpu.VMEM((bl * rl, grid), F32),
                pltpu.VMEM((LANES, LANES), F32),
                pltpu.VMEM((N, 1, LANES), F32),
                pltpu.VMEM((1, 1, LANES), F32),
                dma((phases, C)), dma((phases, C)),
                dma((C - 1,)), dma((C - 1,)),
                dma((N - 1,)), dma((N - 1,)), dma,
                dma((N - 1,)), dma((N - 1,)),
                dma, dma, dma((count,)), dma,
            ],
            compiler_params=pltpu.CompilerParams(
                collective_id=0, has_side_effects=True, vmem_limit_bytes=56 * 1024 * 1024
            ),
        )(orient_bin, tilt_slope, particles, interp_table)
        return pl.pallas_call(
            functools.partial(finish, shells),
            out_shape=(
                jax.ShapeDtypeStruct((1, 2, rl, cl), F32),
                jax.ShapeDtypeStruct((2, shells), F32),
                jax.ShapeDtypeStruct((1, shells), F32),
            ),
            in_specs=[vmem, vmem, vmem],
            out_specs=(vmem, vmem, vmem),
        )(maps, spectra, counts)

    placed = (
        P(("half", "row", "col"), None, None, None),
        P(("half", "row", "col")),
        P(("half", "row", "col"), None),
        P(),
    )
    return jax.shard_map(
        local,
        mesh=mesh,
        in_specs=placed,
        out_specs=(P("half", None, "row", "col"), P(), P("half", None)),
        check_vma=False,
    )
```
